32 devices in a mesh: fsdp: 2 (over x), ctx: 4 (over y, core), tp: 4 (over z).
Axes of the slice: x: 2, y: 2, z: 4, core: 2. Of those that a mesh axis runs over, the one named last changes fastest.
Arguments:
- tokens: bfloat16 [8, 1024, 2048], P('fsdp', 'ctx'), may hold values from -8 to 8
- positions: int32 [8, 1024], P('fsdp', 'ctx'), may hold values from 0 to 383, as said below
- block_ids: int32 [8, 1024], P('fsdp', 'ctx'), may hold values from 0 to 3, as said below
- gain_attend: bfloat16 [2048], P('fsdp'), may hold values from 0.099609375 to 1.8984375
- w_query: bfloat16 [2048, 2048], P('fsdp', 'tp'), may hold values from -0.125 to 0.125
- w_key: bfloat16 [2048, 2048], P('fsdp', 'tp'), may hold values from -0.125 to 0.125
- w_value: bfloat16 [2048, 2048], P('fsdp', 'tp'), may hold values from -0.125 to 0.125
- w_output: bfloat16 [2048, 2048], P('tp', 'fsdp'), may hold values from -1 to 1
- gain_feed: bfloat16 [2048], P('fsdp'), may hold values from 0.099609375 to 1.8984375
- w_gate: bfloat16 [2048, 8192], P('fsdp', 'tp'), may hold values from -0.125 to 0.125
- w_up: bfloat16 [2048, 8192], P('fsdp', 'tp'), may hold values from -0.125 to 0.125
- w_down: bfloat16 [8192, 2048], P('tp', 'fsdp'), may hold values from -0.0625 to 0.0625
- cotangent: bfloat16 [8, 1024, 2048], P('fsdp', 'ctx'), may hold values from -6 to 6
Outputs:
- layer_out: bfloat16 [8, 1024, 2048], P('fsdp', 'ctx')
- grad_input: bfloat16 [8, 1024, 2048], P('fsdp', 'ctx')
- grad_gain_attend: float32 [2048], P(('fsdp', 'ctx'))
- grad_w_query: float32 [2048, 2048], P(('fsdp', 'ctx'), 'tp')
- grad_w_key: float32 [2048, 2048], P(('fsdp', 'ctx'), 'tp')
- grad_w_value: float32 [2048, 2048], P(('fsdp', 'ctx'), 'tp')
- grad_w_output: float32 [2048, 2048], P('tp', ('fsdp', 'ctx'))
- grad_gain_feed: float32 [2048], P(('fsdp', 'ctx'))
- grad_w_gate: float32 [2048, 8192], P(('fsdp', 'ctx'), 'tp')
- grad_w_up: float32 [2048, 8192], P(('fsdp', 'ctx'), 'tp')
- grad_w_down: float32 [8192, 2048], P('tp', ('fsdp', 'ctx'))
- stream_rms: float32 [], replicated
- attend_rms: float32 [], replicated
- feed_rms: float32 [], replicated
The draws below stay inside these ranges and needn't reach their ends.
Inputs may be any that keep to these rules, and one draw needn't show every extreme that they name: Along each sequence, positions count 0, 1, 2 and so on from the first token of each block, a run of equal block ids. `block_ids`: along each sequence block ids start at 0, never fall and rise by one at each new block.
All inputs are finite; a program needn't handle non-finite values.
Results may differ from the reference program's by a relative error of at most 0.015.
Values may be sent and summed in bfloat16 or wider, within the bound.
A program may use at most 256 MiB of HBM per device.

```python
import math
import jax
import jax.numpy as jnp
from jax import lax

D = 2048
HEADS = 16
HD = 128
FF = 8192
BLK = 256
L = 1024
SEQS = 8


def block_layout(key):
    layout_key = jax.random.fold_in(key, 7)
    block_total = L // BLK
    shifts = jax.random.randint(layout_key, (SEQS, block_total - 1), -(BLK // 4), BLK // 4 + 1)
    shifts = shifts.at[0, 0].set(-(BLK // 4)).at[0, 1].set(BLK // 4)
    bounds = (jnp.arange(1, block_total, dtype=jnp.int32) * BLK)[None, :] + shifts
    places = jnp.arange(L, dtype=jnp.int32)
    blocks = jnp.sum((places[None, :, None] >= bounds[:, None, :]).astype(jnp.int32), axis=-1)
    starts = jnp.concatenate([jnp.zeros((SEQS, 1), jnp.int32), bounds.astype(jnp.int32)], axis=1)
    first_place = jnp.take_along_axis(starts, blocks, axis=1)
    return (blocks.astype(jnp.int32), (places[None, :] - first_place).astype(jnp.int32))


def draw_block_ids(key, part):
    blocks, offsets = block_layout(key)
    return blocks


def draw_positions(key, part):
    blocks, offsets = block_layout(key)
    return offsets


def draw_tokens(key, part):
    rising = 0.6 + 1.2 * jnp.arange(SEQS, dtype=jnp.float32) / max(SEQS - 1, 1)
    base = jnp.clip(jax.random.normal(key, (SEQS, L, D), jnp.float32), -4.0, 4.0)
    return (base * rising[:, None, None]).astype(jnp.bfloat16)


def block_levels(stream_key, shape, shards, smallest, largest):
    level, own = 1.0, jax.random.fold_in(stream_key, 6)
    for axis_at, shards_of in shards:
        heights = jnp.exp(jax.random.uniform(jax.random.fold_in(own, axis_at), (shards_of,), jnp.float32, smallest / len(shards), largest / len(shards)))
        level = level * jnp.repeat(heights, shape[axis_at] // shards_of).reshape([-1 if axis == axis_at else 1 for axis in range(len(shape))])
    return level


def centred(stream_key, dims, scale, limit, cuts=(), kind=jnp.bfloat16):
    loudness = block_levels(stream_key, dims, cuts, -0.22, 0.18) if cuts else 1.0
    values = jax.random.normal(stream_key, dims, jnp.float32) * scale * loudness
    return jnp.minimum(jnp.maximum(values, -limit), limit).astype(kind)


def setup_inputs(seed: int = 0) -> dict:
    streams_of = jax.random.split(jax.random.key(seed), 14)
    return {
        "tokens": draw_tokens(jax.random.fold_in(streams_of[13], 71), 0),
        "positions": draw_positions(jax.random.fold_in(streams_of[13], 71), 0),
        "block_ids": draw_block_ids(jax.random.fold_in(streams_of[13], 71), 0),
        "gain_attend": jnp.clip(1.0 + 0.18 * jax.random.normal(streams_of[3], (D,), jnp.float32), 0.099609375, 1.8984375).astype(jnp.bfloat16),
        "w_query": centred(streams_of[4], (D, D), D ** -0.5, 0.125, ((0, 2), (1, 4))),
        "w_key": centred(streams_of[5], (D, D), D ** -0.5, 0.125, ((0, 2), (1, 4))),
        "w_value": centred(streams_of[6], (D, D), D ** -0.5, 0.125, ((0, 2), (1, 4))),
        "w_output": centred(streams_of[7], (D, D), (max(D // 64, 8)) ** -0.5, 1.0, ((0, 4), (1, 2))),
        "gain_feed": jnp.clip(1.0 + 0.18 * jax.random.normal(streams_of[8], (D,), jnp.float32), 0.099609375, 1.8984375).astype(jnp.bfloat16),
        "w_gate": centred(streams_of[9], (D, FF), D ** -0.5, 0.125, ((0, 2), (1, 4))),
        "w_up": centred(streams_of[10], (D, FF), D ** -0.5, 0.125, ((0, 2), (1, 4))),
        "w_down": centred(streams_of[11], (FF, D), FF ** -0.5, 0.0625, ((0, 4), (1, 2))),
        "cotangent": centred(streams_of[12], (SEQS, L, D), 1.0, 6.0, ((0, 2), (1, 4))),
    }


norm_epsilon = 1e-05
rope_base = 10000.0

@jax.custom_vjp
def low(v):
    return lax.optimization_barrier(v.astype(jnp.bfloat16)).astype(jnp.float32)

@jax.custom_vjp
def low_back(v):
    return v

def low_keep(v):
    return (low(v), None)

def low_pass(kept, grad):
    return (grad,)

def back_keep(v):
    return (v, None)

def back_low(kept, grad):
    return (low(grad),)
low.defvjp(low_keep, low_pass)
low_back.defvjp(back_keep, back_low)

def rope_tables(positions, head_size):
    half_size = head_size // 2
    inverse = jnp.exp(jnp.arange(half_size, dtype=jnp.float32) * (-2.0 * math.log(rope_base) / head_size))
    turned = positions.astype(jnp.float32)[..., None, None] * inverse
    return (jnp.cos(turned), jnp.sin(turned))

def rotate(values, cosine, sine_table, direction):
    half_size = values.shape[-1] // 2
    first_half = values[..., :half_size]
    second_half = values[..., half_size:]
    return jnp.concatenate([first_half * cosine - direction * (second_half * sine_table), direction * (first_half * sine_table) + second_half * cosine], axis=-1)

def rms_norm(values, gain):
    return values * lax.rsqrt(lax.optimization_barrier(jnp.mean(values * values, axis=-1, keepdims=True)) + norm_epsilon) * gain

def forward_layer(stream, weights, positions, block_ids):
    gain_one, query_w, key_w, value_w, output_w, gain_two, gate_w, up_w, down_w = weights
    highest = lax.Precision.HIGHEST
    seq_len = stream.shape[0]
    normed_one = low(rms_norm(stream, gain_one))
    queries = low_back(jnp.dot(normed_one, query_w, precision=highest))
    key_proj = low_back(jnp.dot(normed_one, key_w, precision=highest))
    values = low(low_back(jnp.dot(normed_one, value_w, precision=highest)))
    cosine, sine_table = rope_tables(positions, HD)
    query_rot = low(rotate(queries.reshape(seq_len, HEADS, HD), cosine, sine_table, 1.0))
    key_rot = low(rotate(key_proj.reshape(seq_len, HEADS, HD), cosine, sine_table, 1.0))
    value_heads = values.reshape(seq_len, HEADS, HD)
    logits = jnp.einsum('qhd,khd->hqk', query_rot, key_rot, precision=highest) * (1.0 / math.sqrt(HD)) - math.log(L)
    logits = low_back(logits)
    allowed = block_ids[None, :] <= block_ids[:, None]
    probs = low(jnp.where(allowed[None], jax.nn.sigmoid(logits), 0.0))
    mixed = jnp.einsum('hqk,khd->qhd', probs, value_heads, precision=highest).reshape(seq_len, HEADS * HD)
    mixed = low(low_back(mixed))
    attend_out = low_back(jnp.dot(mixed, output_w, precision=highest))
    middle = stream + attend_out
    normed_two = low(rms_norm(middle, gain_two))
    gate_vals = low_back(jnp.dot(normed_two, gate_w, precision=highest))
    up_vals = low_back(jnp.dot(normed_two, up_w, precision=highest))
    hidden = low(jax.nn.silu(gate_vals) * up_vals)
    feed_out = low_back(jnp.dot(hidden, down_w, precision=highest))
    result = middle + feed_out
    return (result, (attend_out, feed_out))

def reference(tokens, positions, block_ids, gain_attend, w_query, w_key, w_value, w_output, gain_feed, w_gate, w_up, w_down, cotangent):
    params = tuple((p.astype(jnp.float32) for p in (gain_attend, w_query, w_key, w_value, w_output, gain_feed, w_gate, w_up, w_down)))

    def per_sequence(carry, sequence):
        gradients, squares = carry
        seq_tokens, seq_positions, seq_blocks, seq_cotangent = sequence

        def forward(stream, *weights):
            return forward_layer(stream, weights, seq_positions, seq_blocks)
        result, pull, branches = jax.vjp(forward, seq_tokens.astype(jnp.float32), *params, has_aux=True)
        pulled = pull(seq_cotangent.astype(jnp.float32))
        gradients = tuple((acc + new_part for acc, new_part in zip(gradients, pulled[1:])))
        attend_out, feed_out = branches
        squares = squares + jnp.stack([jnp.sum(result * result), jnp.sum(attend_out * attend_out), jnp.sum(feed_out * feed_out)])
        return ((gradients, squares), (result.astype(jnp.bfloat16), pulled[0].astype(jnp.bfloat16)))
    start_state = (tuple((jnp.zeros_like(p) for p in params)), jnp.zeros((3,), jnp.float32))
    (gradients, squares), (layer_out, grad_input) = lax.scan(per_sequence, start_state, (tokens, positions, block_ids, cotangent))
    entries = float(SEQS * L * D)
    root_means = jnp.sqrt(squares / entries)
    return (layer_out, grad_input, gradients[0], gradients[1], gradients[2], gradients[3], gradients[4], gradients[5], gradients[6], gradients[7], gradients[8], root_means[0], root_means[1], root_means[2])
```

```python
import math

import jax
import jax.numpy as jnp
from jax import lax
from jax.sharding import PartitionSpec as P

HD = 128


norm_epsilon = 1e-05
rope_base = 10000.0


def plain_dot(left_side, right_side):
    return jnp.dot(left_side, right_side, preferred_element_type=jnp.float32)


def dot_last(left_side, right_side):
    return lax.dot_general(
        left_side, right_side, (((1,), (1,)), ((), ())), preferred_element_type=jnp.float32
    )


def dot_first(left_side, right_side):
    return lax.dot_general(
        left_side, right_side, (((0,), (0,)), ((), ())), preferred_element_type=jnp.float32
    )


def inverse_rms(values):
    return lax.rsqrt(jnp.mean(values * values, axis=-1, keepdims=True) + norm_epsilon)


def norm_back(grad_norm, values, scale_rows, gain):
    weighted = grad_norm * gain
    inner_mean = jnp.mean(weighted * values, axis=-1, keepdims=True)
    grad_values = (
        scale_rows * weighted - values * (scale_rows * scale_rows * scale_rows) * inner_mean
    )
    grad_gain = jnp.sum(grad_norm * (values * scale_rows), axis=0)
    return (grad_values, grad_gain)


def rope_tables(positions, head_size):
    half_size = head_size // 2
    inverse = jnp.exp(
        jnp.arange(half_size, dtype=jnp.float32) * (-2.0 * math.log(rope_base) / head_size)
    )
    turned = positions.astype(jnp.float32)[..., None, None] * inverse
    return (jnp.cos(turned), jnp.sin(turned))


def rotate(values, cosine, sine_table, direction):
    half_size = values.shape[-1] // 2
    first_half = values[..., :half_size]
    second_half = values[..., half_size:]
    return jnp.concatenate(
        [
            first_half * cosine - direction * (second_half * sine_table),
            direction * (first_half * sine_table) + second_half * cosine,
        ],
        axis=-1,
    )


def spread_rows(piece, ctx_size):
    part = piece.shape[0] // ctx_size
    mine = lax.dynamic_slice_in_dim(piece, lax.axis_index("ctx") * part, part, 0)
    return lax.all_gather(mine, ("fsdp", "ctx"), axis=0, tiled=True)


def spread_columns(piece, ctx_size):
    part = piece.shape[0] // ctx_size
    mine = lax.dynamic_slice_in_dim(piece, lax.axis_index("ctx") * part, part, 0)
    held = lax.all_gather(mine, ("fsdp", "ctx"), axis=0, tiled=True)
    fsdp_size = lax.axis_size("fsdp")
    held = held.reshape(fsdp_size, piece.shape[0], piece.shape[1])
    return jnp.swapaxes(held, 0, 1).reshape(piece.shape[0], fsdp_size * piece.shape[1])


def sum_rows(partial):
    return lax.psum_scatter(
        partial.astype(jnp.bfloat16), "tp", scatter_dimension=0, tiled=True
    ).astype(jnp.float32)


def every_row(rows):
    return lax.all_gather(rows, "tp", axis=0, tiled=True)


def local(
    tokens,
    positions,
    block_ids,
    gain_attend,
    w_query,
    w_key,
    w_value,
    w_output,
    gain_feed,
    w_gate,
    w_up,
    w_down,
    cotangent,
):
    seq_count, block_len, model_width = tokens.shape
    row_count = seq_count * block_len
    ctx_size = lax.axis_size("ctx")
    tp_size = lax.axis_size("tp")
    seq_len = block_len * ctx_size
    heads_here = w_query.shape[1] // HD
    width_here = heads_here * HD
    score_scale = 1.0 / math.sqrt(HD)
    score_shift = math.log(seq_len)
    shape_heads = (seq_count, block_len, heads_here, HD)
    low = jnp.bfloat16
    part_rows = row_count // tp_size
    row_at = lax.axis_index("tp") * part_rows

    token_rows = tokens.reshape(row_count, model_width)
    grad_rows = cotangent.reshape(row_count, model_width)
    token_part = lax.dynamic_slice_in_dim(token_rows, row_at, part_rows, 0).astype(jnp.float32)
    cotangent_part = lax.dynamic_slice_in_dim(grad_rows, row_at, part_rows, 0).astype(jnp.float32)

    qkv_full = spread_rows(jnp.concatenate([w_query, w_key, w_value], axis=1), ctx_size)
    gains = lax.all_gather(jnp.stack([gain_attend, gain_feed]), "fsdp", axis=1, tiled=True)
    gain_one = gains[0].astype(jnp.float32)
    gain_two = gains[1].astype(jnp.float32)
    output_full = spread_columns(w_output, ctx_size)
    gate_full = spread_rows(w_gate, ctx_size)
    up_full = spread_rows(w_up, ctx_size)
    down_full = spread_columns(w_down, ctx_size)

    stream = token_rows.astype(jnp.float32)
    scale_one = inverse_rms(stream)
    normed_one = (stream * scale_one * gain_one).astype(low)
    projected = plain_dot(normed_one, qkv_full)
    queries = projected[:, :width_here]
    key_proj = projected[:, width_here : 2 * width_here]
    values = projected[:, 2 * width_here :].astype(low)
    cosine, sine_table = rope_tables(positions, HD)
    query_rot = rotate(queries.reshape(shape_heads), cosine, sine_table, 1.0).astype(low)
    key_rot = rotate(key_proj.reshape(shape_heads), cosine, sine_table, 1.0).astype(low)

    key_value = lax.all_gather(
        jnp.concatenate(
            [
                key_rot.reshape(seq_count, block_len, width_here),
                values.reshape(seq_count, block_len, width_here),
            ],
            axis=2,
        ),
        "ctx",
        axis=1,
        tiled=True,
    )
    key_tags = lax.all_gather(block_ids, "ctx", axis=1, tiled=True)
    key_heads = key_value[:, :, :width_here].reshape(seq_count, seq_len, heads_here, HD)
    value_heads = key_value[:, :, width_here:].reshape(seq_count, seq_len, heads_here, HD)
    logits = (
        jnp.einsum("sqhd,skhd->shqk", query_rot, key_heads, preferred_element_type=jnp.float32)
        * score_scale
        - score_shift
    )
    allowed = key_tags[:, None, None, :] <= block_ids[:, None, :, None]
    squashed = jax.nn.sigmoid(logits)
    weights = jnp.where(allowed, squashed, 0.0).astype(low)
    attended = jnp.einsum(
        "shqk,skhd->sqhd", weights, value_heads, preferred_element_type=jnp.float32
    )
    mixed_rows = attended.reshape(row_count, width_here).astype(low)

    attend_part = sum_rows(plain_dot(mixed_rows, output_full))
    middle = token_part + attend_part
    scale_two = inverse_rms(middle)
    normed_two = every_row((middle * scale_two * gain_two).astype(low))

    gate_vals = plain_dot(normed_two, gate_full)
    up_vals = plain_dot(normed_two, up_full)
    gate_sig = jax.nn.sigmoid(gate_vals)
    gate_act = gate_vals * gate_sig
    hidden = (gate_act * up_vals).astype(low)
    grad_hidden = dot_last(grad_rows, down_full)
    slope = gate_sig * (1.0 + gate_vals * (1.0 - gate_sig))
    grad_gate = (grad_hidden * up_vals * slope).astype(low)
    grad_up = (grad_hidden * gate_act).astype(low)
    grad_normed_two = sum_rows(dot_last(grad_gate, gate_full) + dot_last(grad_up, up_full))

    feed_part = sum_rows(plain_dot(hidden, down_full))
    result = middle + feed_part
    layer_out = every_row(result.astype(low)).reshape(tokens.shape)

    grad_middle_norm, grad_gain_two = norm_back(grad_normed_two, middle, scale_two, gain_two)
    grad_middle = cotangent_part + grad_middle_norm
    grad_attend = every_row(grad_middle.astype(low))

    def scatter(value, dimension):
        return lax.psum_scatter(
            value.astype(low), ("fsdp", "ctx"), scatter_dimension=dimension, tiled=True
        ).astype(jnp.float32)

    grad_down = scatter(dot_first(hidden, grad_rows), 1)
    grad_gate_w = scatter(dot_first(normed_two, grad_gate), 0)
    grad_up_w = scatter(dot_first(normed_two, grad_up), 0)

    grad_mixed = dot_last(grad_attend, output_full).astype(low)
    grad_output_w = scatter(dot_first(mixed_rows, grad_attend), 1)
    grad_mixed_heads = grad_mixed.reshape(shape_heads)
    grad_weights = jnp.einsum(
        "sqhd,skhd->shqk", grad_mixed_heads, value_heads, preferred_element_type=jnp.float32
    )
    grad_logits = jnp.where(allowed, grad_weights * squashed * (1.0 - squashed), 0.0).astype(low)
    grad_query = score_scale * jnp.einsum(
        "shqk,skhd->sqhd", grad_logits, key_heads, preferred_element_type=jnp.float32
    )
    key_part = score_scale * jnp.einsum(
        "shqk,sqhd->skhd", grad_logits, query_rot, preferred_element_type=jnp.float32
    )
    value_part = jnp.einsum(
        "shqk,sqhd->skhd", weights, grad_mixed_heads, preferred_element_type=jnp.float32
    )
    pair = jnp.concatenate(
        [
            key_part.reshape(seq_count, seq_len, width_here).astype(low),
            value_part.reshape(seq_count, seq_len, width_here).astype(low),
        ],
        axis=2,
    )
    mine = lax.psum_scatter(pair, "ctx", scatter_dimension=1, tiled=True).astype(jnp.float32)
    grad_query_rows = rotate(grad_query, cosine, sine_table, -1.0).reshape(row_count, width_here)
    grad_key_rows = rotate(
        mine[:, :, :width_here].reshape(shape_heads), cosine, sine_table, -1.0
    ).reshape(row_count, width_here)
    grad_qkv = jnp.concatenate(
        [
            grad_query_rows.astype(low),
            grad_key_rows.astype(low),
            mine[:, :, width_here:].reshape(row_count, width_here).astype(low),
        ],
        axis=1,
    )
    grad_normed_one = sum_rows(dot_last(grad_qkv, qkv_full))
    grad_qkv_w = scatter(dot_first(normed_one, grad_qkv), 0)
    scale_one_part = lax.dynamic_slice_in_dim(scale_one, row_at, part_rows, 0)
    grad_input_norm, grad_gain_one = norm_back(
        grad_normed_one, token_part, scale_one_part, gain_one
    )
    grad_input = every_row((grad_middle + grad_input_norm).astype(low)).reshape(tokens.shape)

    sums = jnp.stack(
        [jnp.sum(result * result), jnp.sum(attend_part * attend_part), jnp.sum(feed_part * feed_part)]
    )
    small = lax.psum(
        jnp.concatenate([grad_gain_one, grad_gain_two, sums]), ("fsdp", "ctx", "tp")
    )
    shards = lax.axis_size("fsdp") * ctx_size
    entries = float(row_count * model_width * shards)
    roots = jnp.sqrt(small[2 * model_width :] / entries)
    gain_part = model_width // shards
    gain_at = (lax.axis_index("fsdp") * ctx_size + lax.axis_index("ctx")) * gain_part
    grad_gain_attend = lax.dynamic_slice_in_dim(small, gain_at, gain_part, 0)
    grad_gain_feed = lax.dynamic_slice_in_dim(small, model_width + gain_at, gain_part, 0)
    return (
        layer_out,
        grad_input,
        grad_gain_attend,
        grad_qkv_w[:, :width_here],
        grad_qkv_w[:, width_here : 2 * width_here],
        grad_qkv_w[:, 2 * width_here :],
        grad_output_w,
        grad_gain_feed,
        grad_gate_w,
        grad_up_w,
        grad_down,
        roots[0],
        roots[1],
        roots[2],
    )


def solution(mesh):
    placed = (
        P("fsdp", "ctx", None),
        P("fsdp", "ctx"),
        P("fsdp", "ctx"),
        P("fsdp"),
        P("fsdp", "tp"),
        P("fsdp", "tp"),
        P("fsdp", "tp"),
        P("tp", "fsdp"),
        P("fsdp"),
        P("fsdp", "tp"),
        P("fsdp", "tp"),
        P("tp", "fsdp"),
        P("fsdp", "ctx", None),
    )
    return jax.shard_map(
        local,
        mesh=mesh,
        in_specs=placed,
        out_specs=(
            P("fsdp", "ctx", None),
            P("fsdp", "ctx", None),
            P(("fsdp", "ctx")),
            P(("fsdp", "ctx"), "tp"),
            P(("fsdp", "ctx"), "tp"),
            P(("fsdp", "ctx"), "tp"),
            P("tp", ("fsdp", "ctx")),
            P(("fsdp", "ctx")),
            P(("fsdp", "ctx"), "tp"),
            P(("fsdp", "ctx"), "tp"),
            P("tp", ("fsdp", "ctx")),
            P(),
            P(),
            P(),
        ),
        check_vma=False,
    )
```

```python
import math

import jax
import jax.numpy as jnp
from jax import lax
from jax.experimental import pallas as pl
from jax.experimental.pallas import tpu as pltpu
from jax.sharding import PartitionSpec as P

HD = 128


norm_epsilon = 1e-05
rope_base = 10000.0


def plain_dot(left_side, right_side):
    return jnp.dot(left_side, right_side, preferred_element_type=jnp.float32)


def dot_last(left_side, right_side):
    return lax.dot_general(
        left_side, right_side, (((1,), (1,)), ((), ())), preferred_element_type=jnp.float32
    )


def dot_first(left_side, right_side):
    return lax.dot_general(
        left_side, right_side, (((0,), (0,)), ((), ())), preferred_element_type=jnp.float32
    )


def inverse_rms(values):
    return lax.rsqrt(jnp.mean(values * values, axis=-1, keepdims=True) + norm_epsilon)


def norm_back(grad_norm, values, scale_rows, gain):
    weighted = grad_norm * gain
    inner_mean = jnp.mean(weighted * values, axis=-1, keepdims=True)
    grad_values = (
        scale_rows * weighted - values * (scale_rows * scale_rows * scale_rows) * inner_mean
    )
    grad_gain = jnp.sum(grad_norm * (values * scale_rows), axis=0)
    return (grad_values, grad_gain)


def rope_tables(positions, head_size):
    half_size = head_size // 2
    inverse = jnp.exp(
        jnp.arange(half_size, dtype=jnp.float32) * (-2.0 * math.log(rope_base) / head_size)
    )
    turned = positions.astype(jnp.float32)[..., None, None] * inverse
    return (jnp.cos(turned), jnp.sin(turned))


def rotate(values, cosine, sine_table, direction):
    half_size = values.shape[-1] // 2
    first_half = values[..., :half_size]
    second_half = values[..., half_size:]
    return jnp.concatenate(
        [
            first_half * cosine - direction * (second_half * sine_table),
            direction * (first_half * sine_table) + second_half * cosine,
        ],
        axis=-1,
    )


def spread_rows(piece, ctx_size):
    part = piece.shape[0] // ctx_size
    mine = lax.dynamic_slice_in_dim(piece, lax.axis_index("ctx") * part, part, 0)
    return lax.all_gather(mine, ("fsdp", "ctx"), axis=0, tiled=True)


def spread_columns(piece, ctx_size):
    part = piece.shape[0] // ctx_size
    mine = lax.dynamic_slice_in_dim(piece, lax.axis_index("ctx") * part, part, 0)
    held = lax.all_gather(mine, ("fsdp", "ctx"), axis=0, tiled=True)
    fsdp_size = lax.axis_size("fsdp")
    held = held.reshape(fsdp_size, piece.shape[0], piece.shape[1])
    return jnp.swapaxes(held, 0, 1).reshape(piece.shape[0], fsdp_size * piece.shape[1])


CHUNK = 32
GROUP = 4
TILE = 512
VMEM_BYTES = 66000000
MESH_ID = pl.DeviceIdType.MESH


def chunk_rows(index, rows=CHUNK):
    return pl.ds(pl.multiple_of(index * rows, rows), rows)


def fold_rows(values):
    return jnp.sum(values.reshape(values.shape[0] // 8, 8, values.shape[1]), axis=0)


class Line:
    def __init__(self, size, chunks, own, held, out, sems):
        self.size, self.chunks, self.own, self.held, self.out, self.sems = (
            size,
            chunks,
            own,
            held,
            out,
            sems,
        )
        self.rank = lax.axis_index("tp")
        self.is_end = (self.rank == 0) | (self.rank == size - 1)
        self.end_half = jnp.where(self.rank == 0, 0, 1)

    def enter(self):
        barrier = pltpu.get_barrier_semaphore()
        rank, size = self.rank, self.size

        @pl.when(rank > 0)
        def _():
            pl.semaphore_signal(
                barrier, inc=1, device_id={"tp": rank - 1}, device_id_type=MESH_ID
            )

        @pl.when(rank < size - 1)
        def _():
            pl.semaphore_signal(
                barrier, inc=1, device_id={"tp": rank + 1}, device_id_type=MESH_ID
            )

        pl.semaphore_wait(barrier, jnp.where(self.is_end, 1, 2))

    def place(self, half):
        rank, size = self.rank, self.size
        if half == 0:
            return size - 1 - rank, jnp.maximum(rank - 1, 0), jnp.minimum(rank + 1, size - 1)
        return rank, jnp.minimum(rank + 1, size - 1), jnp.maximum(rank - 1, 0)

    def send_on(self, half, chunk, target, first):
        rows = chunk_rows(chunk)
        source = self.own if first else self.held
        return pltpu.make_async_remote_copy(
            src_ref=source.at[half, rows],
            dst_ref=self.held.at[half, rows],
            send_sem=self.sems.at[0, half, chunk],
            recv_sem=self.sems.at[1, half, chunk],
            device_id={"tp": target},
            device_id_type=MESH_ID,
        )

    def send_back(self, half, chunk, target):
        rows = chunk_rows(chunk)
        return pltpu.make_async_remote_copy(
            src_ref=self.out.at[half, rows],
            dst_ref=self.out.at[half, rows],
            send_sem=self.sems.at[2, half, chunk],
            recv_sem=self.sems.at[3, half, chunk],
            device_id={"tp": target},
            device_id_type=MESH_ID,
        )

    def slot(self, step, finish, arrived):
        last = self.size - 1
        for half in (0, 1):
            place, onward, back = self.place(half)
            chunk = step - place
            rows = chunk_rows(chunk)

            @pl.when((chunk >= 0) & (chunk < self.chunks) & (place == 0))
            def _():
                self.send_on(half, chunk, onward, True).start()

            @pl.when((chunk >= 0) & (chunk < self.chunks) & (place > 0) & (place < last))
            def _():
                self.send_on(half, chunk, onward, False).wait_recv()
                total = self.held[half, rows].astype(jnp.float32) + self.own[half, rows].astype(
                    jnp.float32
                )
                self.held[half, rows] = total.astype(jnp.bfloat16)
                self.send_on(half, chunk, onward, False).start()

            @pl.when((chunk >= 0) & (chunk < self.chunks) & (place == last))
            def _():
                self.send_on(half, chunk, onward, False).wait_recv()

        chunk = step - last
        rows = chunk_rows(chunk)

        @pl.when((chunk >= 0) & (chunk < self.chunks) & self.is_end)
        def _():
            half = self.end_half
            total = self.held[half, rows].astype(jnp.float32) + self.own[half, rows].astype(
                jnp.float32
            )
            finish(chunk, total)
            inward = jnp.where(self.rank == 0, 1, last - 1)
            self.send_back(half, chunk, inward).start()
            arrived(half, chunk)

        for half in (0, 1):
            place, onward, back = self.place(half)
            chunk = step - last - (last - place)

            @pl.when((chunk >= 0) & (chunk < self.chunks) & (place < last))
            def _():
                self.send_back(half, chunk, back).wait_recv()

                @pl.when(place > 0)
                def _():
                    self.send_back(half, chunk, back).start()

                arrived(half, chunk)

    def leave(self):
        last = self.size - 1

        @pl.loop(0, self.chunks)
        def _(chunk):
            for half in (0, 1):
                place, onward, back = self.place(half)

                @pl.when(place < last)
                def _():
                    self.send_on(half, chunk, onward, True).wait_send()

                @pl.when(place > 0)
                def _():
                    self.send_back(half, chunk, back).wait_send()


def load_all(pairs, sems):
    return [
        pltpu.make_async_copy(source, target, sems.at[index])
        for index, (source, target) in enumerate(pairs)
    ]


def feed_kernel(
    size,
    partial,
    tokens,
    cotangent,
    gate,
    up,
    down,
    gain,
    normed_out,
    hidden_out,
    grad_gate_out,
    grad_up_out,
    middle_out,
    square_out,
    own,
    held,
    out,
    stream,
    cot,
    gate_in,
    up_in,
    down_in,
    middle,
    staged,
    sems,
    load_sems,
    save_sems,
    stage_sems,
    middle_sem,
):
    half_rows = own.shape[1]
    chunks = half_rows // CHUNK
    width = gate_in.shape[1]
    tiles = width // TILE
    group_rows = GROUP * CHUNK
    groups = chunks // GROUP
    line = Line(size, chunks, own, held, out, sems)
    half = line.end_half
    loads = load_all(
        [
            (partial, own),
            (tokens.at[half], stream),
            (cotangent, cot),
            (gate, gate_in),
            (up, up_in),
            (down, down_in),
        ],
        load_sems,
    )
    for load in loads:
        load.start()
    square_out[...] = jnp.zeros_like(square_out)
    line.enter()
    loads[0].wait()
    loads[1].wait()

    def finish(chunk, total):
        rows = chunk_rows(chunk)
        mid = stream[rows].astype(jnp.float32) + total
        square_out[...] += fold_rows(total * total)
        middle[rows] = mid
        out[half, rows] = (mid * inverse_rms(mid) * gain[...]).astype(jnp.bfloat16)

    def save(which, chunk):
        rows = chunk_rows(chunk)
        return pltpu.make_async_copy(
            out.at[which, rows], normed_out.at[which, rows], save_sems.at[which, chunk]
        )

    def arrived(which, chunk):
        save(which, chunk).start()

    def stage(index, which, slot, group, tile):
        target = (hidden_out, grad_gate_out, grad_up_out)[index]
        return pltpu.make_async_copy(
            staged.at[slot, index, which],
            target.at[which, chunk_rows(group, group_rows), chunk_rows(tile, TILE)],
            stage_sems.at[slot, index, which],
        )

    head = 2 * (size - 1) + GROUP - 1
    units = groups * tiles

    @pl.loop(0, head + max(chunks, units) + 1)
    def _(step):
        line.slot(step, finish, arrived)
        unit = step - head

        @pl.when(unit == 0)
        def _():
            for load in loads[2:]:
                load.wait()

        @pl.when((unit >= 0) & (unit < units))
        def _():
            group = unit // tiles
            tile = unit % tiles
            slot = unit % 2
            group_at = chunk_rows(group, group_rows)
            tile_at = chunk_rows(tile, TILE)

            @pl.when(unit >= 2)
            def _():
                for index in range(3):
                    for which in (0, 1):
                        stage(index, which, slot, group, tile).wait()

            rows = out[:, group_at].reshape(2 * group_rows, out.shape[2])
            outer = cot[:, group_at].reshape(2 * group_rows, out.shape[2])
            gate_vals = plain_dot(rows, gate_in[:, tile_at])
            up_vals = plain_dot(rows, up_in[:, tile_at])
            grad_hidden = dot_last(outer, down_in[tile_at])
            gate_sig = jax.nn.sigmoid(gate_vals)
            gate_act = gate_vals * gate_sig
            slope = gate_sig * (1.0 + gate_vals * (1.0 - gate_sig))
            made = (gate_act * up_vals, grad_hidden * up_vals * slope, grad_hidden * gate_act)
            for index in range(3):
                staged[slot, index] = (
                    made[index].astype(jnp.bfloat16).reshape(2, group_rows, TILE)
                )
                for which in (0, 1):
                    stage(index, which, slot, group, tile).start()

    @pl.when(line.is_end)
    def _():
        pltpu.make_async_copy(middle, middle_out, middle_sem).start()

    @pl.loop(0, chunks)
    def _(chunk):
        for which in (0, 1):
            save(which, chunk).wait()

    for slot in (0, 1):
        for index in range(3):
            for which in (0, 1):
                stage(index, which, slot, 0, 0).wait()
    line.leave()

    @pl.when(line.is_end)
    def _():
        pltpu.make_async_copy(middle, middle_out, middle_sem).wait()


def feed_block(partial, tokens, cotangent, gate, up, down, gain, size):
    rows, model_width = partial.shape
    half_rows = rows // 2
    width = gate.shape[1]
    low = jnp.bfloat16
    chunks = half_rows // CHUNK
    anywhere = pl.BlockSpec(memory_space=pl.ANY)
    local_spec = pl.BlockSpec(memory_space=pltpu.VMEM)
    halves = (2, half_rows, model_width)
    hidden_shape = jax.ShapeDtypeStruct((2, half_rows, width), low)
    outs = pl.pallas_call(
        lambda *refs: feed_kernel(size, *refs),
        out_shape=(
            jax.ShapeDtypeStruct(halves, low),
            hidden_shape,
            hidden_shape,
            hidden_shape,
            jax.ShapeDtypeStruct((half_rows, model_width), jnp.float32),
            jax.ShapeDtypeStruct((8, model_width), jnp.float32),
        ),
        in_specs=[anywhere] * 6 + [local_spec],
        out_specs=[anywhere] * 5 + [local_spec],
        scratch_shapes=[
            pltpu.VMEM(halves, low),
            pltpu.VMEM(halves, low),
            pltpu.VMEM(halves, low),
            pltpu.VMEM((half_rows, model_width), low),
            pltpu.VMEM(halves, low),
            pltpu.VMEM(gate.shape, low),
            pltpu.VMEM(up.shape, low),
            pltpu.VMEM(down.shape, low),
            pltpu.VMEM((half_rows, model_width), jnp.float32),
            pltpu.VMEM((2, 3, 2, GROUP * CHUNK, TILE), low),
            pltpu.SemaphoreType.DMA((4, 2, chunks)),
            pltpu.SemaphoreType.DMA((6,)),
            pltpu.SemaphoreType.DMA((2, chunks)),
            pltpu.SemaphoreType.DMA((2, 3, 2)),
            pltpu.SemaphoreType.DMA(()),
        ],
        compiler_params=pltpu.CompilerParams(
            collective_id=1, has_side_effects=True, vmem_limit_bytes=VMEM_BYTES
        ),
        cost_estimate=pl.CostEstimate(
            flops=6 * rows * model_width * width, bytes_accessed=300000000, transcendentals=0
        ),
        name="feed_block",
    )(
        partial.reshape(halves),
        tokens.reshape(halves),
        cotangent.reshape(halves),
        gate,
        up,
        down,
        gain.reshape(1, model_width),
    )
    normed, hidden, grad_gate, grad_up, middle, squares = outs
    flat = (rows, width)
    return (
        normed.reshape(rows, model_width),
        hidden.reshape(flat),
        grad_gate.reshape(flat),
        grad_up.reshape(flat),
        middle,
        squares,
    )


def back_kernel(
    size,
    hidden,
    grad_gate,
    grad_up,
    gate,
    up,
    down,
    cotangent,
    middle,
    gain,
    attend_out,
    layer_out,
    grad_middle_out,
    sum_out,
    own,
    held,
    out,
    gate_in,
    up_in,
    down_in,
    left,
    cot,
    mid,
    grad_mid,
    sems,
    load_sems,
    left_sems,
    end_sems,
    save_sems,
):
    half_rows = hidden.shape[1]
    chunks = half_rows // CHUNK
    model_width = gate_in.shape[0]
    tiles = model_width // TILE
    group_rows = GROUP * CHUNK
    groups = chunks // GROUP
    last = size - 1
    line = Line(size, 2 * chunks, own, held, out, sems)
    half = line.end_half
    loads = load_all([(gate, gate_in), (up, up_in), (down, down_in)], load_sems)
    for load in loads:
        load.start()

    def fetch(source, group, slot, place):
        rows = chunk_rows(lax.rem(group, groups), group_rows)
        return pltpu.make_async_copy(
            source.at[:, rows], left.at[slot, place], left_sems.at[slot, place]
        )

    def start_fetch(group):
        slot = lax.rem(group, 2)

        @pl.when(group < groups)
        def _():
            fetch(grad_gate, group, slot, 0).start()
            fetch(grad_up, group, slot, 1).start()

        @pl.when((group >= groups) & (group < 2 * groups))
        def _():
            fetch(hidden, group, slot, 0).start()

    def make(group, tile):
        slot = lax.rem(group, 2)
        tile_at = chunk_rows(tile, TILE)
        rows_at = chunk_rows(group, group_rows)

        @pl.when(tile == 0)
        def _():
            @pl.when(group < groups)
            def _():
                fetch(grad_gate, group, slot, 0).wait()
                fetch(grad_up, group, slot, 1).wait()

            @pl.when(group >= groups)
            def _():
                fetch(hidden, group, slot, 0).wait()

            start_fetch(group + 1)

        shape = (2 * group_rows, left.shape[4])

        @pl.when(group < groups)
        def _():
            total = dot_last(left[slot, 0].reshape(shape), gate_in[tile_at]) + dot_last(
                left[slot, 1].reshape(shape), up_in[tile_at]
            )
            own[:, rows_at, tile_at] = total.astype(jnp.bfloat16).reshape(2, group_rows, TILE)

        @pl.when(group >= groups)
        def _():
            total = plain_dot(left[slot, 0].reshape(shape), down_in[:, tile_at])
            own[:, rows_at, tile_at] = total.astype(jnp.bfloat16).reshape(2, group_rows, TILE)

    def fetch_end(chunk, slot):
        rows = chunk_rows(lax.rem(chunk, chunks))
        return (
            pltpu.make_async_copy(middle.at[rows], mid.at[slot], end_sems.at[slot, 0]),
            pltpu.make_async_copy(cotangent.at[half, rows], cot.at[slot], end_sems.at[slot, 1]),
        )

    def grad_save(chunk, slot):
        return pltpu.make_async_copy(
            grad_mid.at[slot], grad_middle_out.at[chunk_rows(chunk)], end_sems.at[slot, 2]
        )

    start_fetch(0)
    sum_out[...] = jnp.zeros_like(sum_out)
    line.enter()
    loads[0].wait()
    loads[1].wait()

    @pl.when(line.is_end)
    def _():
        for copy in fetch_end(0, 0):
            copy.start()

    @pl.loop(0, tiles)
    def _(tile):
        make(0, tile)

    loads[2].wait()

    def finish(chunk, total):
        slot = lax.rem(chunk, 2)
        for copy in fetch_end(chunk, slot):
            copy.wait()

        @pl.when(chunk + 1 < 2 * chunks)
        def _():
            for copy in fetch_end(chunk + 1, 1 - slot):
                copy.start()

        mids = mid[slot]
        rows = chunk_rows(chunk)

        @pl.when(chunk < chunks)
        def _():
            scale = inverse_rms(mids)
            weighted = total * gain[...]
            inner = jnp.mean(weighted * mids, axis=-1, keepdims=True)
            grad = (
                cot[slot].astype(jnp.float32)
                + scale * weighted
                - mids * (scale * scale * scale * inner)
            )
            sum_out[0] += fold_rows(total * (mids * scale))
            out[half, rows] = grad.astype(jnp.bfloat16)

            @pl.when(chunk >= 2)
            def _():
                grad_save(chunk - 2, slot).wait()

            grad_mid[slot] = grad
            grad_save(chunk, slot).start()

        @pl.when(chunk >= chunks)
        def _():
            result = mids + total
            sum_out[1] += fold_rows(result * result)
            sum_out[2] += fold_rows(total * total)
            out[half, rows] = result.astype(jnp.bfloat16)

    def save(which, chunk, target):
        rows = chunk_rows(lax.rem(chunk, chunks))
        return pltpu.make_async_copy(
            out.at[which, chunk_rows(chunk)],
            target.at[which, rows],
            save_sems.at[which, chunk],
        )

    def arrived(which, chunk):
        @pl.when(chunk < chunks)
        def _():
            save(which, chunk, attend_out).start()

        @pl.when(chunk >= chunks)
        def _():
            save(which, chunk, layer_out).start()

    @pl.loop(0, 2 * chunks + 2 * last)
    def _(step):
        line.slot(step, finish, arrived)
        unit = step + tiles

        @pl.when(unit < 2 * groups * tiles)
        def _():
            make(unit // tiles, unit % tiles)

    @pl.loop(0, chunks)
    def _(chunk):
        for which in (0, 1):
            save(which, chunk, attend_out).wait()
            save(which, chunk + chunks, layer_out).wait()

    @pl.when(line.is_end)
    def _():
        for chunk in (chunks - 2, chunks - 1):
            grad_save(chunk, chunk % 2).wait()

    line.leave()


def back_block(hidden, grad_gate, grad_up, gate, up, down, cotangent, middle, gain, size):
    rows, width = hidden.shape
    model_width = gate.shape[0]
    half_rows = rows // 2
    low = jnp.bfloat16
    chunks = half_rows // CHUNK
    anywhere = pl.BlockSpec(memory_space=pl.ANY)
    local_spec = pl.BlockSpec(memory_space=pltpu.VMEM)
    halves = (2, half_rows, model_width)
    hidden_halves = (2, half_rows, width)
    both = (2, 2 * half_rows, model_width)
    grad_attend, layer, grad_middle, sums = pl.pallas_call(
        lambda *refs: back_kernel(size, *refs),
        out_shape=(
            jax.ShapeDtypeStruct(halves, low),
            jax.ShapeDtypeStruct(halves, low),
            jax.ShapeDtypeStruct((half_rows, model_width), jnp.float32),
            jax.ShapeDtypeStruct((3, 8, model_width), jnp.float32),
        ),
        in_specs=[anywhere] * 8 + [local_spec],
        out_specs=[anywhere] * 3 + [local_spec],
        scratch_shapes=[
            pltpu.VMEM(both, low),
            pltpu.VMEM(both, low),
            pltpu.VMEM(both, low),
            pltpu.VMEM(gate.shape, low),
            pltpu.VMEM(up.shape, low),
            pltpu.VMEM(down.shape, low),
            pltpu.VMEM((2, 2, 2, GROUP * CHUNK, width), low),
            pltpu.VMEM((2, CHUNK, model_width), low),
            pltpu.VMEM((2, CHUNK, model_width), jnp.float32),
            pltpu.VMEM((2, CHUNK, model_width), jnp.float32),
            pltpu.SemaphoreType.DMA((4, 2, 2 * chunks)),
            pltpu.SemaphoreType.DMA((3,)),
            pltpu.SemaphoreType.DMA((2, 2)),
            pltpu.SemaphoreType.DMA((2, 3)),
            pltpu.SemaphoreType.DMA((2, 2 * chunks)),
        ],
        compiler_params=pltpu.CompilerParams(
            collective_id=2, has_side_effects=True, vmem_limit_bytes=VMEM_BYTES
        ),
        cost_estimate=pl.CostEstimate(
            flops=6 * rows * model_width * width, bytes_accessed=600000000, transcendentals=0
        ),
        name="back_block",
    )(
        hidden.reshape(hidden_halves),
        grad_gate.reshape(hidden_halves),
        grad_up.reshape(hidden_halves),
        gate,
        up,
        down,
        cotangent.reshape(halves),
        middle,
        gain.reshape(1, model_width),
    )
    return (
        grad_attend.reshape(rows, model_width),
        layer.reshape(rows, model_width),
        grad_middle,
        sums,
    )


def input_kernel(
    size,
    partial,
    tokens,
    grad_middle,
    gain,
    grad_out,
    sum_out,
    own,
    held,
    out,
    stream,
    grad_mid,
    sems,
    load_sems,
    save_sems,
):
    half_rows = own.shape[1]
    chunks = half_rows // CHUNK
    line = Line(size, chunks, own, held, out, sems)
    half = line.end_half
    loads = load_all(
        [(partial, own), (tokens.at[half], stream), (grad_middle, grad_mid)], load_sems
    )
    for load in loads:
        load.start()
    sum_out[...] = jnp.zeros_like(sum_out)
    line.enter()
    for load in loads:
        load.wait()

    def finish(chunk, total):
        rows = chunk_rows(chunk)
        values = stream[rows].astype(jnp.float32)
        scale = inverse_rms(values)
        weighted = total * gain[...]
        inner = jnp.mean(weighted * values, axis=-1, keepdims=True)
        grad = grad_mid[rows] + scale * weighted - values * (scale * scale * scale * inner)
        sum_out[...] += fold_rows(total * (values * scale))
        out[half, rows] = grad.astype(jnp.bfloat16)

    def save(which, chunk):
        rows = chunk_rows(chunk)
        return pltpu.make_async_copy(
            out.at[which, rows], grad_out.at[which, rows], save_sems.at[which, chunk]
        )

    def arrived(which, chunk):
        save(which, chunk).start()

    @pl.loop(0, chunks + 2 * (size - 1))
    def _(step):
        line.slot(step, finish, arrived)

    @pl.loop(0, chunks)
    def _(chunk):
        for which in (0, 1):
            save(which, chunk).wait()

    line.leave()


def input_block(partial, tokens, grad_middle, gain, size):
    rows, model_width = partial.shape
    half_rows = rows // 2
    low = jnp.bfloat16
    chunks = half_rows // CHUNK
    anywhere = pl.BlockSpec(memory_space=pl.ANY)
    local_spec = pl.BlockSpec(memory_space=pltpu.VMEM)
    halves = (2, half_rows, model_width)
    grad_input, sums = pl.pallas_call(
        lambda *refs: input_kernel(size, *refs),
        out_shape=(
            jax.ShapeDtypeStruct(halves, low),
            jax.ShapeDtypeStruct((8, model_width), jnp.float32),
        ),
        in_specs=[anywhere] * 3 + [local_spec],
        out_specs=[anywhere, local_spec],
        scratch_shapes=[
            pltpu.VMEM(halves, low),
            pltpu.VMEM(halves, low),
            pltpu.VMEM(halves, low),
            pltpu.VMEM((half_rows, model_width), low),
            pltpu.VMEM((half_rows, model_width), jnp.float32),
            pltpu.SemaphoreType.DMA((4, 2, chunks)),
            pltpu.SemaphoreType.DMA((3,)),
            pltpu.SemaphoreType.DMA((2, chunks)),
        ],
        compiler_params=pltpu.CompilerParams(
            collective_id=3, has_side_effects=True, vmem_limit_bytes=VMEM_BYTES
        ),
        cost_estimate=pl.CostEstimate(flops=0, bytes_accessed=300000000, transcendentals=0),
        name="input_block",
    )(
        partial.reshape(halves),
        tokens.reshape(halves),
        grad_middle,
        gain.reshape(1, model_width),
    )
    return grad_input.reshape(rows, model_width), sums


def local(
    tokens,
    positions,
    block_ids,
    gain_attend,
    w_query,
    w_key,
    w_value,
    w_output,
    gain_feed,
    w_gate,
    w_up,
    w_down,
    cotangent,
):
    seq_count, block_len, model_width = tokens.shape
    row_count = seq_count * block_len
    ctx_size = lax.axis_size("ctx")
    tp_size = lax.axis_size("tp")
    seq_len = block_len * ctx_size
    heads_here = w_query.shape[1] // HD
    width_here = heads_here * HD
    score_scale = 1.0 / math.sqrt(HD)
    score_shift = math.log(seq_len)
    shape_heads = (seq_count, block_len, heads_here, HD)
    low = jnp.bfloat16

    token_rows = tokens.reshape(row_count, model_width)
    grad_rows = cotangent.reshape(row_count, model_width)

    qkv_full = spread_rows(jnp.concatenate([w_query, w_key, w_value], axis=1), ctx_size)
    gains = lax.all_gather(jnp.stack([gain_attend, gain_feed]), "fsdp", axis=1, tiled=True)
    gain_one = gains[0].astype(jnp.float32)
    gain_two = gains[1].astype(jnp.float32)
    output_full = spread_columns(w_output, ctx_size)
    gate_full = spread_rows(w_gate, ctx_size)
    up_full = spread_rows(w_up, ctx_size)
    down_full = spread_columns(w_down, ctx_size)

    stream = token_rows.astype(jnp.float32)
    scale_one = inverse_rms(stream)
    normed_one = (stream * scale_one * gain_one).astype(low)
    projected = plain_dot(normed_one, qkv_full)
    queries = projected[:, :width_here]
    key_proj = projected[:, width_here : 2 * width_here]
    values = projected[:, 2 * width_here :].astype(low)
    cosine, sine_table = rope_tables(positions, HD)
    query_rot = rotate(queries.reshape(shape_heads), cosine, sine_table, 1.0).astype(low)
    key_rot = rotate(key_proj.reshape(shape_heads), cosine, sine_table, 1.0).astype(low)

    key_value = lax.all_gather(
        jnp.concatenate(
            [
                key_rot.reshape(seq_count, block_len, width_here),
                values.reshape(seq_count, block_len, width_here),
            ],
            axis=2,
        ),
        "ctx",
        axis=1,
        tiled=True,
    )
    key_tags = lax.all_gather(block_ids, "ctx", axis=1, tiled=True)
    key_heads = key_value[:, :, :width_here].reshape(seq_count, seq_len, heads_here, HD)
    value_heads = key_value[:, :, width_here:].reshape(seq_count, seq_len, heads_here, HD)
    logits = (
        jnp.einsum("sqhd,skhd->shqk", query_rot, key_heads, preferred_element_type=jnp.float32)
        * score_scale
        - score_shift
    )
    allowed = key_tags[:, None, None, :] <= block_ids[:, None, :, None]
    squashed = jax.nn.sigmoid(logits)
    weights = jnp.where(allowed, squashed, 0.0).astype(low)
    attended = jnp.einsum(
        "shqk,skhd->sqhd", weights, value_heads, preferred_element_type=jnp.float32
    )
    mixed_rows = attended.reshape(row_count, width_here).astype(low)

    attend_part = plain_dot(mixed_rows, output_full).astype(low)
    normed_two, hidden, grad_gate, grad_up, middle, attend_squares = feed_block(
        attend_part, token_rows, grad_rows, gate_full, up_full, down_full, gain_two, tp_size
    )

    def scatter(value, dimension):
        return lax.psum_scatter(
            value.astype(low), ("fsdp", "ctx"), scatter_dimension=dimension, tiled=True
        ).astype(jnp.float32)

    grad_down = scatter(dot_first(hidden, grad_rows), 1)
    grad_gate_w = scatter(dot_first(normed_two, grad_gate), 0)
    grad_up_w = scatter(dot_first(normed_two, grad_up), 0)

    grad_attend, layer_rows, grad_middle, feed_sums = back_block(
        hidden,
        grad_gate,
        grad_up,
        gate_full,
        up_full,
        down_full,
        grad_rows,
        middle,
        gain_two,
        tp_size,
    )
    layer_out = layer_rows.reshape(tokens.shape)

    grad_mixed = dot_last(grad_attend, output_full).astype(low)
    grad_output_w = scatter(dot_first(mixed_rows, grad_attend), 1)
    grad_mixed_heads = grad_mixed.reshape(shape_heads)
    grad_weights = jnp.einsum(
        "sqhd,skhd->shqk", grad_mixed_heads, value_heads, preferred_element_type=jnp.float32
    )
    grad_logits = jnp.where(allowed, grad_weights * squashed * (1.0 - squashed), 0.0).astype(low)
    grad_query = score_scale * jnp.einsum(
        "shqk,skhd->sqhd", grad_logits, key_heads, preferred_element_type=jnp.float32
    )
    key_part = score_scale * jnp.einsum(
        "shqk,sqhd->skhd", grad_logits, query_rot, preferred_element_type=jnp.float32
    )
    value_part = jnp.einsum(
        "shqk,sqhd->skhd", weights, grad_mixed_heads, preferred_element_type=jnp.float32
    )
    pair = jnp.concatenate(
        [
            key_part.reshape(seq_count, seq_len, width_here).astype(low),
            value_part.reshape(seq_count, seq_len, width_here).astype(low),
        ],
        axis=2,
    )
    mine = lax.psum_scatter(pair, "ctx", scatter_dimension=1, tiled=True).astype(jnp.float32)
    grad_query_rows = rotate(grad_query, cosine, sine_table, -1.0).reshape(row_count, width_here)
    grad_key_rows = rotate(
        mine[:, :, :width_here].reshape(shape_heads), cosine, sine_table, -1.0
    ).reshape(row_count, width_here)
    grad_qkv = jnp.concatenate(
        [
            grad_query_rows.astype(low),
            grad_key_rows.astype(low),
            mine[:, :, width_here:].reshape(row_count, width_here).astype(low),
        ],
        axis=1,
    )
    grad_qkv_w = scatter(dot_first(normed_one, grad_qkv), 0)
    input_rows, input_sums = input_block(
        dot_last(grad_qkv, qkv_full).astype(low), token_rows, grad_middle, gain_one, tp_size
    )
    grad_input = input_rows.reshape(tokens.shape)

    grad_gain_one = jnp.sum(input_sums, axis=0)
    grad_gain_two = jnp.sum(feed_sums[0], axis=0)
    sums = jnp.stack([jnp.sum(feed_sums[1]), jnp.sum(attend_squares), jnp.sum(feed_sums[2])])
    small = lax.psum(
        jnp.concatenate([grad_gain_one, grad_gain_two, sums]), ("fsdp", "ctx", "tp")
    )
    shards = lax.axis_size("fsdp") * ctx_size
    entries = float(row_count * model_width * shards)
    roots = jnp.sqrt(small[2 * model_width :] / entries)
    gain_part = model_width // shards
    gain_at = (lax.axis_index("fsdp") * ctx_size + lax.axis_index("ctx")) * gain_part
    grad_gain_attend = lax.dynamic_slice_in_dim(small, gain_at, gain_part, 0)
    grad_gain_feed = lax.dynamic_slice_in_dim(small, model_width + gain_at, gain_part, 0)
    return (
        layer_out,
        grad_input,
        grad_gain_attend,
        grad_qkv_w[:, :width_here],
        grad_qkv_w[:, width_here : 2 * width_here],
        grad_qkv_w[:, 2 * width_here :],
        grad_output_w,
        grad_gain_feed,
        grad_gate_w,
        grad_up_w,
        grad_down,
        roots[0],
        roots[1],
        roots[2],
    )


def solution(mesh):
    placed = (
        P("fsdp", "ctx", None),
        P("fsdp", "ctx"),
        P("fsdp", "ctx"),
        P("fsdp"),
        P("fsdp", "tp"),
        P("fsdp", "tp"),
        P("fsdp", "tp"),
        P("tp", "fsdp"),
        P("fsdp"),
        P("fsdp", "tp"),
        P("fsdp", "tp"),
        P("tp", "fsdp"),
        P("fsdp", "ctx", None),
    )
    return jax.shard_map(
        local,
        mesh=mesh,
        in_specs=placed,
        out_specs=(
            P("fsdp", "ctx", None),
            P("fsdp", "ctx", None),
            P(("fsdp", "ctx")),
            P(("fsdp", "ctx"), "tp"),
            P(("fsdp", "ctx"), "tp"),
            P(("fsdp", "ctx"), "tp"),
            P("tp", ("fsdp", "ctx")),
            P(("fsdp", "ctx")),
            P(("fsdp", "ctx"), "tp"),
            P(("fsdp", "ctx"), "tp"),
            P("tp", ("fsdp", "ctx")),
            P(),
            P(),
            P(),
        ),
        check_vma=False,
    )
```
